32 devices in a mesh: bin: 4 (over y, core), tile: 8 (over z, x).
Axes of the slice: x: 2, y: 2, z: 4, core: 2. Of those that a mesh axis runs over, the one named last changes fastest.
Arguments:
- shear_one: float32 [4, 4096, 4096], P('bin', 'tile'), may hold values from -6 to 6
- shear_two: float32 [4, 4096, 4096], P('bin', 'tile'), may hold values from -6 to 6
- weights: float32 [4, 4], replicated, may hold values from 0.2 to 1
Outputs:
- convergence: float32 [4, 4096, 4096], P('bin', 'tile')
The draws below stay inside these ranges and needn't reach their ends.
All inputs are finite; a program needn't handle non-finite values.
Results may differ from the reference program's by a relative error of at most 0.000071.
Values sent between devices are 32-bit elements; how exact they have to be, the bound alone decides.
No kernel may reach another device: no remote copies, remote signals or barrier semaphores. Data moves between devices by JAX's collectives and lax.ppermute only.
A program may use at most 128 MiB of HBM per device.

```python
import math
import jax
import jax.numpy as jnp
from jax import lax

N = 4096
BINS = 4


def steps_of(key, shape, pieces, smallest, high):
    level = 1.0
    for position, parts in pieces:
        heights = jax.random.uniform(jax.random.fold_in(jax.random.fold_in(key, 6), position), (parts,), jnp.float32, smallest / len(pieces), high / len(pieces))
        level = level * jnp.repeat(jnp.exp(heights), shape[position] // parts).reshape((-1,) + (1,) * (len(shape) - 1 - position))
    return level


def bell_draw(own_key, extent, spread, limit, pieces=(), kind=jnp.bfloat16):
    gain = steps_of(own_key, extent, pieces, -0.22, 0.18) if pieces else 1.0
    entries = jax.random.normal(own_key, extent, jnp.float32) * spread * gain
    return jnp.minimum(jnp.maximum(entries, -limit), limit).astype(kind)


def setup_inputs(seed: int = 0) -> dict:
    streams_of = jax.random.split(jax.random.key(seed), 4)
    shear_one = bell_draw(streams_of[0], (BINS, N, N), 1.0, 6.0, ((0, 4), (1, 8)), jnp.float32)
    shear_two = bell_draw(streams_of[1], (BINS, N, N), 1.0, 6.0, ((0, 4), (1, 8)), jnp.float32)
    weights = jnp.clip(jnp.exp(jax.random.uniform(streams_of[2], (BINS, BINS), jnp.float32, math.log(0.2), math.log(1.0))), 0.2, 1.0)
    return dict(shear_one=shear_one, shear_two=shear_two, weights=weights)


def signed_frequency(length):
    index = jnp.arange(length, dtype=jnp.int32)
    return jnp.where(index < length // 2, index, index - length)


def reference(shear_one, shear_two, weights):
    length = shear_one.shape[-1]
    frequency = signed_frequency(length)
    row_freq = frequency[:, None]
    col_freq = frequency[None, :]
    radius = col_freq * col_freq + row_freq * row_freq
    radius_floor = jnp.maximum(radius, 1).astype(jnp.float32)
    kern_real = (col_freq * col_freq - row_freq * row_freq).astype(jnp.float32) / radius_floor
    kern_imag = (2 * col_freq * row_freq).astype(jnp.float32) / radius_floor

    def convert(shears):
        spectrum = jnp.fft.fft2(lax.complex(shears[0], shears[1]))
        spec_real = jnp.real(spectrum)
        spec_imag = jnp.imag(spectrum)
        new_real = kern_real * spec_real + kern_imag * spec_imag
        new_imag = kern_real * spec_imag - kern_imag * spec_real
        return jnp.real(jnp.fft.ifft2(lax.complex(new_real, new_imag)))

    fields = lax.map(convert, (shear_one, shear_two))
    order_index = jnp.arange(weights.shape[0], dtype=jnp.int32)
    masked = jnp.where(order_index[:, None] >= order_index[None, :], weights, jnp.zeros_like(weights))
    return jnp.einsum("ji,irc->jrc", masked, fields, precision=lax.Precision.HIGHEST)
```

```python
import functools

import jax
import jax.numpy as jnp
import ml_dtypes
import numpy as np
from jax import lax
from jax.experimental import pallas as pl
from jax.experimental.pallas import tpu as pltpu
from jax.sharding import PartitionSpec as P

LANES = 128
SUBLANES = 8
CHUNKS = 2


def complex_times(real, imag, factor):
    fr, fi = factor.real, factor.imag
    if abs(fi) < 1e-12:
        fr = round(fr) if abs(abs(fr) - 1) < 1e-12 else fr
        if fr == 1:
            return real, imag
        if fr == -1:
            return -real, None if imag is None else -imag
        return real * fr, None if imag is None else imag * fr
    if abs(fr) < 1e-12:
        sign = 1 if fi > 0 else -1
        if imag is None:
            return None, real if sign > 0 else -real
        return (-imag, real) if sign > 0 else (imag, -real)
    if imag is None:
        return real * fr, real * fi
    if abs(abs(fr) - abs(fi)) < 1e-12:
        size, sr, si = abs(fr), fr > 0, fi > 0
        re = (real - imag) if sr == si else (real + imag)
        im = (real + imag) if sr == si else (imag - real)
        if sr and si:
            return re * size, im * size
        if not sr and not si:
            return re * -size, im * -size
        if sr:
            return re * size, im * size
        return re * -size, im * -size
    return real * fr - imag * fi, real * fi + imag * fr


def plus(a, b):
    return b if a is None else a if b is None else a + b


def minus(a, b):
    return a if b is None else -b if a is None else a - b


def full_transform(values, orient):
    size = len(values)
    if size == 1:
        return values
    even = full_transform(values[0::2], orient)
    odd = full_transform(values[1::2], orient)
    half = size // 2
    out = [None] * size
    for k in range(half):
        tr, ti = complex_times(*odd[k], np.exp(orient * 2j * np.pi * k / size))
        er, ei = even[k]
        out[k] = (plus(er, tr), plus(ei, ti))
        out[k + half] = (minus(er, tr), minus(ei, ti))
    return out


def real_transform(values):
    size = len(values)
    if size == 2:
        return [(values[0] + values[1], None), (values[0] - values[1], None)]
    even = real_transform(values[0::2])
    odd = real_transform(values[1::2])
    half = size // 2
    out = [None] * (half + 1)
    for k in range(size // 4 + 1):
        tr, ti = complex_times(*odd[k], np.exp(-2j * np.pi * k / size))
        er, ei = even[k]
        low = minus(ei, ti)
        out[half - k] = (minus(er, tr), None if low is None else -low)
        out[k] = (plus(er, tr), plus(ei, ti))
    return out


def real_inverse(spectrum):
    size = 2 * (len(spectrum) - 1)
    if size == 2:
        return [spectrum[0][0] + spectrum[1][0], spectrum[0][0] - spectrum[1][0]]
    half = size // 2
    even, odd = [], []
    for k in range(size // 4 + 1):
        ar, ai = spectrum[k]
        br, bi = spectrum[half - k]
        if k == size // 4:
            even.append((ar + ar, None))
            odd.append((-(ai + ai), None))
            continue
        er, ei = plus(ar, br), minus(ai, bi)
        dr, di = minus(ar, br), plus(ai, bi)
        if k == 0:
            ei = di = None
        even.append((er, ei))
        odd.append(complex_times(dr, di, np.exp(2j * np.pi * k / size)))
    out = [None] * size
    out[0::2] = real_inverse(even)
    out[1::2] = real_inverse(odd)
    return out


def halves(matrix):
    high = matrix.astype(ml_dtypes.bfloat16)
    low = (matrix - high.astype(np.float64)).astype(ml_dtypes.bfloat16)
    return np.stack([high, low])


def column_places(narrow, chunks):
    wide = narrow // chunks
    chunk, holder, part, column = np.meshgrid(
        np.arange(chunks), np.arange(LANES // narrow), np.arange(2), np.arange(wide), indexing="ij"
    )
    return part.reshape(-1), (holder * narrow + chunk * wide + column).reshape(-1)


def lane_transform(orient):
    index = np.arange(LANES)
    angle = orient * 2 * np.pi * np.outer(index, index) / LANES
    cos, sin = np.cos(angle), np.sin(angle)
    return np.block([[cos, sin], [-sin, cos]])


def row_matrices(length, narrow, chunks):
    pieces = length // LANES
    part, column = column_places(narrow, chunks)
    q = np.arange(LANES)
    angle = 2 * np.pi * np.outer(column, q) / LANES
    cos, sin = np.cos(angle), np.sin(angle)
    real = (part == 0)[:, None]
    forward = np.where(real, np.hstack([cos, sin]), np.hstack([-sin, cos]))
    inverse = np.where(real, np.hstack([cos, sin]), np.hstack([-sin, cos]))
    late = (column >= LANES // 2)[:, None]
    within = np.where(column >= LANES // 2, column - LANES // 2, column)
    angle = 2 * np.pi * (np.outer(within, q) / LANES + late * (pieces // 2) * q[None, :] / length)
    wave = np.where(real, np.cos(angle), -np.sin(angle))
    first = (column == 0)[:, None]
    wave = np.where(first & ~real, 1.0 - 2.0 * (q % 2)[None, :], wave)
    zero = np.zeros_like(wave)
    edge_forward = np.where(late, np.hstack([zero, wave]), np.hstack([wave, zero]))
    edge_inverse = edge_forward * np.where(first, 1.0, 2.0)
    return halves(forward), halves(inverse), halves(edge_forward), halves(edge_inverse)


def twiddle(length):
    pieces = length // LANES
    angle = 2 * np.pi * np.outer(np.arange(pieces), np.arange(LANES)) / length
    table = np.stack([np.cos(angle), np.sin(angle)]).astype(np.float32)
    return np.ascontiguousarray(
        np.broadcast_to(table[:, :, None, :], (2, pieces, SUBLANES, LANES))
    )


def parts_of(values):
    high = values.astype(jnp.bfloat16)
    low = (values - high.astype(jnp.float32)).astype(jnp.bfloat16)
    return high, low


def product(left, right, dims):
    dot = functools.partial(
        lax.dot_general, dimension_numbers=(dims, ((), ())), preferred_element_type=jnp.float32
    )
    return dot(left[0], right[0]) + dot(left[0], right[1]) + dot(left[1], right[0])


def rows_kernel(one_ref, two_ref, matrix_ref, edge_ref, twiddle_ref, *refs):
    *out_refs, mid_ref = refs
    rows = one_ref.shape[0]
    blocks = mid_ref.shape[0]
    pieces = 2 * blocks
    chunks = len(out_refs)
    holders, wide = out_refs[0].shape[1], out_refs[0].shape[4]

    for field, ref in enumerate((one_ref, two_ref)):

        def over_pieces(step, carry, ref=ref):
            at = pl.ds(pl.multiple_of(step * SUBLANES, SUBLANES), SUBLANES)
            values = [ref[at, p * LANES : (p + 1) * LANES] for p in range(pieces)]
            spectrum = real_transform(values)
            mid_ref[0, at, :LANES] = spectrum[0][0]
            mid_ref[0, at, LANES:] = spectrum[blocks][0]
            for k in range(1, blocks):
                real, imag = spectrum[k]
                cos, sin = twiddle_ref[0, k], twiddle_ref[1, k]
                mid_ref[k, at, :LANES] = real * cos + imag * sin
                mid_ref[k, at, LANES:] = imag * cos - real * sin
            return carry

        lax.fori_loop(0, rows // SUBLANES, over_pieces, 0)

        def over_lanes(k, matrix_ref, field=field):
            result = product(
                (matrix_ref[0], matrix_ref[1]), parts_of(mid_ref[k]), (((1,), (1,)))
            )
            at = 0
            for chunk in range(chunks):
                for holder in range(holders):
                    for part in range(2):
                        out_refs[chunk][k, holder, field, part] = result[at : at + wide]
                        at += wide

        over_lanes(0, edge_ref)

        def each(k, carry, over_lanes=over_lanes):
            over_lanes(k, matrix_ref)
            return carry

        lax.fori_loop(1, blocks, each, 0)


def columns_kernel(
    flag_ref, weights_ref, in_ref, freq_ref, forward_ref, inverse_ref, twiddle_ref, out_ref, mid_ref, hat_ref, two_ref
):
    total_bins = weights_ref.shape[0]
    tiles = in_ref.shape[0] // total_bins
    span = in_ref.shape[4] // LANES
    pieces = tiles * span
    length = pieces * LANES
    special = jnp.logical_and(flag_ref[0] == 1, pl.program_id(0) == 0)
    sublane = lax.broadcasted_iota(jnp.int32, (SUBLANES, LANES), 0)
    lane = lax.broadcasted_iota(jnp.int32, (SUBLANES, LANES), 1)
    packed = jnp.logical_and(sublane == 0, special)
    col_freq = freq_ref[...]

    def factors(k, col_freq):
        index = lane * pieces + k
        row_freq = jnp.where(index < length // 2, index, index - length).astype(jnp.float32)
        col_sq, row_sq = col_freq * col_freq, row_freq * row_freq
        floor = jnp.maximum(col_sq + row_sq, 1.0)
        return (col_sq - row_sq) / floor, 2.0 * col_freq * row_freq / floor

    def store_mid(spectrum, orient):
        for k, (real, imag) in enumerate(spectrum):
            at = slice(k * SUBLANES, (k + 1) * SUBLANES)
            if k == 0:
                mid_ref[at, :LANES] = real
                mid_ref[at, LANES:] = imag
                continue
            cos, sin = twiddle_ref[0, k], twiddle_ref[1, k]
            mid_ref[at, :LANES] = real * cos + imag * sin
            mid_ref[at, LANES:] = imag * cos - real * sin

    def forward_of(bin_at, field):
        values = []
        for p in range(pieces):
            at = bin_at * tiles + p // span
            cut = slice((p % span) * LANES, (p % span + 1) * LANES)
            real = in_ref[at, field, 0, :, cut]
            imag = in_ref[at, field, 1, :, cut]
            if field == 0:
                imag = jnp.where(packed, 0.0, imag)
            else:
                real = jnp.where(packed, 0.0, real)
                imag = jnp.where(packed, in_ref[at, 0, 1, :, cut], imag)
            values.append((real, imag))
        store_mid(full_transform(values, -1), -1)
        return product(parts_of(mid_ref[...]), (forward_ref[0], forward_ref[1]), ((1,), (0,)))

    def each_bin(bin_at, carry):
        one = forward_of(bin_at, 0)
        hat_ref[bin_at] = one
        two_ref[...] = forward_of(bin_at, 1)

        for k in range(pieces):
            at = slice(k * SUBLANES, (k + 1) * SUBLANES)
            kern_real, kern_imag = factors(k, col_freq)
            one_real, one_imag = hat_ref[bin_at, at, :LANES], hat_ref[bin_at, at, LANES:]
            two_real, two_imag = two_ref[at, :LANES], two_ref[at, LANES:]
            hat_real = kern_real * one_real + kern_imag * two_real
            hat_imag = kern_real * one_imag + kern_imag * two_imag
            if k == 0:
                middle = lane == LANES // 2
                hat_real = jnp.where(middle, kern_real * one_real + kern_imag * one_imag, hat_real)
                hat_imag = jnp.where(middle, kern_real * one_imag - kern_imag * one_real, hat_imag)
            hat_ref[bin_at, at, :LANES] = hat_real
            hat_ref[bin_at, at, LANES:] = hat_imag

        @pl.when(special)
        def _():
            total = jnp.zeros((SUBLANES, LANES), jnp.float32)
            for p in range(pieces):
                cut = slice((p % span) * LANES, (p % span + 1) * LANES)
                total = total + in_ref[bin_at * tiles + p // span, 1, 1, :, cut]
            signed = jnp.where(lane % 2 == 0, total, -total)
            corner = jnp.sum(signed, axis=1, keepdims=True)
            edge_freq = jnp.full((SUBLANES, LANES), -(length // 2), jnp.float32)
            for k in range(pieces):
                at = slice(k * SUBLANES, (k + 1) * SUBLANES)
                kern_real, kern_imag = factors(k, edge_freq)
                two_real, two_imag = two_ref[at, :LANES], two_ref[at, LANES:]
                add_real = kern_real * two_real + kern_imag * two_imag
                add_imag = kern_real * two_imag - kern_imag * two_real
                if k == 0:
                    middle = lane == LANES // 2
                    add_real = jnp.where(middle, 0.0, add_real)
                    add_imag = jnp.where(middle, jnp.broadcast_to(corner, add_imag.shape), add_imag)
                hat_ref[bin_at, at, :LANES] += jnp.where(sublane == 0, add_real, 0.0)
                hat_ref[bin_at, at, LANES:] += jnp.where(sublane == 0, add_imag, 0.0)

        return carry

    lax.fori_loop(0, total_bins, each_bin, 0)

    def each_source(source, carry):
        summed = weights_ref[source, 0] * hat_ref[0]
        for bin_at in range(1, total_bins):
            summed = summed + weights_ref[source, bin_at] * hat_ref[bin_at]
        mid_ref[...] = product(parts_of(summed), (inverse_ref[0], inverse_ref[1]), ((1,), (0,)))
        values = []
        for k in range(pieces):
            at = slice(k * SUBLANES, (k + 1) * SUBLANES)
            real, imag = mid_ref[at, :LANES], mid_ref[at, LANES:]
            if k:
                cos, sin = twiddle_ref[0, k], twiddle_ref[1, k]
                real, imag = real * cos - imag * sin, imag * cos + real * sin
            values.append((real, imag))
        for p, (real, imag) in enumerate(full_transform(values, 1)):
            at = source * tiles + p // span
            cut = slice((p % span) * LANES, (p % span + 1) * LANES)
            out_ref[at, 0, :, cut] = real
            out_ref[at, 1, :, cut] = imag
        return carry

    lax.fori_loop(0, total_bins, each_source, 0)


def back_kernel(*refs):
    *in_refs, matrix_ref, edge_ref, twiddle_ref, out_ref, mid_ref = refs
    rows = out_ref.shape[0]
    blocks = mid_ref.shape[0]
    pieces = 2 * blocks
    holders = in_refs[0].shape[1]

    def over_lanes(k, matrix_ref):
        slabs = [ref[k, holder, part] for ref in in_refs for holder in range(holders) for part in range(2)]
        values = jnp.concatenate(slabs, axis=0).T
        mid_ref[k] = product(parts_of(values), (matrix_ref[0], matrix_ref[1]), ((1,), (0,)))

    over_lanes(0, edge_ref)

    def each(k, carry):
        over_lanes(k, matrix_ref)
        return carry

    lax.fori_loop(1, blocks, each, 0)

    def over_pieces(step, carry):
        at = pl.ds(pl.multiple_of(step * SUBLANES, SUBLANES), SUBLANES)
        spectrum = [(mid_ref[0, at, :LANES], None)]
        for k in range(1, blocks):
            real, imag = mid_ref[k, at, :LANES], mid_ref[k, at, LANES:]
            cos, sin = twiddle_ref[0, k], twiddle_ref[1, k]
            spectrum.append((real * cos - imag * sin, imag * cos + real * sin))
        spectrum.append((mid_ref[0, at, LANES:], None))
        for p, value in enumerate(real_inverse(spectrum)):
            out_ref[at, p * LANES : (p + 1) * LANES] = value
        return carry

    lax.fori_loop(0, rows // SUBLANES, over_pieces, 0)


def whole(shape):
    return pl.BlockSpec(shape, lambda i: (0,) * len(shape))


def on_device(shear_one, shear_two, weights):
    bins_here, rows, length = shear_one.shape
    total_bins = weights.shape[0]
    tiles = lax.axis_size("tile")
    holders_all = lax.axis_size("bin") * tiles
    pieces = length // LANES
    blocks = pieces // 2
    narrow = length // 2 // holders_all
    wide = narrow // CHUNKS
    holders = LANES // narrow
    assert bins_here == 1 and wide % SUBLANES == 0 and rows % LANES == 0
    step_rows = min(rows, 2 * LANES)
    limit = pltpu.CompilerParams(vmem_limit_bytes=56 * 1024 * 1024)

    forward, inverse, edge_forward, edge_inverse = row_matrices(length, narrow, CHUNKS)
    table = twiddle(length)
    order_index = jnp.arange(total_bins, dtype=jnp.int32)
    masked = jnp.where(
        order_index[:, None] >= order_index[None, :], weights, jnp.zeros_like(weights)
    )

    matrix_shape = (2, 2 * LANES, 2 * LANES)
    shear_spec = pl.BlockSpec((step_rows, length), lambda i: (i, 0))
    sent = pl.pallas_call(
        rows_kernel,
        name="rows_forward",
        grid=(rows // step_rows,),
        in_specs=[shear_spec, shear_spec, whole(matrix_shape), whole(matrix_shape), whole(table.shape)],
        out_specs=[
            pl.BlockSpec((blocks, holders, 2, 2, wide, step_rows), lambda i: (0, 0, 0, 0, 0, i))
        ] * CHUNKS,
        out_shape=[jax.ShapeDtypeStruct((blocks, holders, 2, 2, wide, rows), jnp.float32)] * CHUNKS,
        scratch_shapes=[pltpu.VMEM((blocks, step_rows, 2 * LANES), jnp.float32)],
        compiler_params=limit,
    )(shear_one[0], shear_two[0], forward, edge_forward, table)

    device = lax.axis_index("bin") * tiles + lax.axis_index("tile")
    column = device * narrow + jnp.arange(narrow, dtype=jnp.int32)
    block, within = column // LANES, column % LANES
    edge = jnp.where(within < LANES // 2, within * pieces, (within - LANES // 2) * pieces + blocks)
    frequency = jnp.where(block == 0, edge, block + pieces * within)
    signed = jnp.where(frequency < length // 2, frequency, frequency - length)
    col_freq = jnp.broadcast_to(signed.astype(jnp.float32)[:, None], (narrow, LANES))
    first = (device == 0).astype(jnp.int32)

    to_frequency = halves(lane_transform(-1))
    to_rows = halves(lane_transform(1) / float(length) ** 2)
    returned = []
    for chunk in range(CHUNKS):
        got = lax.all_to_all(
            sent[chunk].reshape(holders_all, 2, 2, wide, rows),
            ("bin", "tile"), split_axis=0, concat_axis=0, tiled=True,
        )
        flag = jnp.reshape(first if chunk == 0 else jnp.zeros_like(first), (1,))
        back = pl.pallas_call(
            columns_kernel,
            name="columns",
            grid=(wide // SUBLANES,),
            in_specs=[
                pl.BlockSpec(memory_space=pltpu.SMEM),
                pl.BlockSpec(memory_space=pltpu.SMEM),
                pl.BlockSpec((holders_all, 2, 2, SUBLANES, rows), lambda i: (0, 0, 0, i, 0)),
                pl.BlockSpec((SUBLANES, LANES), lambda i: (i, 0)),
                whole(matrix_shape),
                whole(matrix_shape),
                whole(table.shape),
            ],
            out_specs=pl.BlockSpec((holders_all, 2, SUBLANES, rows), lambda i: (0, 0, i, 0)),
            out_shape=jax.ShapeDtypeStruct((holders_all, 2, wide, rows), jnp.float32),
            scratch_shapes=[
                pltpu.VMEM((pieces * SUBLANES, 2 * LANES), jnp.float32),
                pltpu.VMEM((total_bins, pieces * SUBLANES, 2 * LANES), jnp.float32),
                pltpu.VMEM((pieces * SUBLANES, 2 * LANES), jnp.float32),
            ],
            compiler_params=limit,
        )(flag, masked, got, col_freq[chunk * wide : (chunk + 1) * wide], to_frequency, to_rows, table)
        returned.append(
            lax.all_to_all(back, ("bin", "tile"), split_axis=0, concat_axis=0, tiled=True)
            .reshape(blocks, holders, 2, wide, rows)
        )

    field = pl.pallas_call(
        back_kernel,
        name="rows_back",
        grid=(rows // step_rows,),
        in_specs=[
            pl.BlockSpec((blocks, holders, 2, wide, step_rows), lambda i: (0, 0, 0, 0, i))
        ] * CHUNKS + [whole(matrix_shape), whole(matrix_shape), whole(table.shape)],
        out_specs=pl.BlockSpec((step_rows, length), lambda i: (i, 0)),
        out_shape=jax.ShapeDtypeStruct((rows, length), jnp.float32),
        scratch_shapes=[pltpu.VMEM((blocks, step_rows, 2 * LANES), jnp.float32)],
        compiler_params=limit,
    )(*returned, inverse, edge_inverse, table)
    return field[None]


def solution(mesh):
    in_specs = (P("bin", "tile", None), P("bin", "tile", None), P())
    out_specs = P("bin", "tile", None)
    return jax.shard_map(
        on_device, mesh=mesh, in_specs=in_specs, out_specs=out_specs, check_vma=False
    )
```
